32 devices in a mesh: dp: 4 (over x, y), tp: 8 (over z, core).
Axes of the slice: x: 2, y: 2, z: 4, core: 2. Of those that a mesh axis runs over, the one named last changes fastest.
Arguments:
- x: bfloat16 [5120, 7168], P(('dp', 'tp')), parts along dimension 0
- dy: bfloat16 [5120, 7168], P(('dp', 'tp')), parts along dimension 0
- pre: bfloat16 [5120, 28672], P('dp', 'tp'), parts along dimension 0
- w_in: bfloat16 [7168, 28672], P(None, 'tp')
- w_down: bfloat16 [28672, 7168], P('tp')
Outputs:
- output 1: bfloat16 [5120, 7168], P(('dp', 'tp')), parts along dimension 0
- output 2: bfloat16 [28672, 28672], P('dp', 'tp'), parts along dimension 0
- output 3: bfloat16 [114688, 7168], P(('dp', 'tp')), parts along dimension 0
There are 4 independent parts. The reference program is written for one: setup_inputs(seed, part) draws one part's arguments, and reference() takes and returns one part's arrays. A program takes and returns all parts, laid end to end along the dimension named above; an argument that names none is the same for every part.
All inputs are finite; a program needn't handle non-finite values.
Results may differ from the reference program's by a relative error of at most 0.012.
Values are sent between devices in bfloat16 or wider.
A program may use at most 2 GiB of HBM per device.

```python
import jax
import jax.numpy as jnp

ROWS = 1280
D = 7168
FF = 28672


def act(pre):
    return jax.nn.gelu(pre)


def setup_inputs(seed: int = 0, part: int = 0) -> dict:
    kx, ky, ka, ki, kd = jax.random.split(jax.random.key(seed), 5)
    kx, ky, ka = (jax.random.fold_in(k, part) for k in (kx, ky, ka))
    drawn = {
        "x": jax.random.normal(kx, (ROWS, D), jnp.float32),
        "dy": jax.random.normal(ky, (ROWS, D), jnp.float32),
        "pre": jax.random.normal(ka, (ROWS, FF), jnp.float32),
        "w_in": jax.random.normal(ki, (D, FF), jnp.float32) * D**-0.5,
        "w_down": jax.random.normal(kd, (FF, D), jnp.float32) * FF**-0.5,
    }
    return {k: v.astype(jnp.bfloat16) for k, v in drawn.items()}


def reference(x, dy, pre, w_in, w_down):
    hidden, back = jax.vjp(act, pre.astype(jnp.float32))
    d_hidden = jnp.dot(dy, w_down.T, preferred_element_type=jnp.float32)
    d_pre = back(d_hidden)[0].astype(jnp.bfloat16)
    dx = jnp.dot(d_pre, w_in.T, preferred_element_type=jnp.float32)
    dw_in = jnp.dot(x.T, d_pre, preferred_element_type=jnp.float32)
    dw_down = jnp.dot(hidden.astype(jnp.bfloat16).T, dy, preferred_element_type=jnp.float32)
    return tuple(g.astype(jnp.bfloat16) for g in (dx, dw_in, dw_down))
```

```python
import functools

import jax
import jax.numpy as jnp
from jax import lax
from jax.experimental import pallas as pl
from jax.experimental.pallas import tpu as pltpu
from jax.sharding import PartitionSpec as P

F32, BF16 = jnp.float32, jnp.bfloat16
NT = (((1,), (1,)), ((), ()))
TN = (((0,), (0,)), ((), ()))
G = 7
STRIP = 16
SLOTS = 4
VMEM = 67043328
PIECES = 3
C0 = 0.7978845608028654
C1 = 0.044715


def gather_reduce_kernel(
    dy, pre, w_in, w_down, dy_all, d_pre, hidden, dx,
    dyv, ring, dpre, hid, preb, held, precv, psend, crecv, cs,
    acc, ws, ios, prs, ls, lr, ps, pr, pss, psr, css, csr, credit,
):
    R, D = dy.shape
    F = pre.shape[1]
    CH, T = D // G, F // G
    t = lax.axis_index("tp")
    z, c = t // 2, t % 2
    partner = t + 1 - 2 * c

    def rows(s, core):
        return pl.ds(pl.multiple_of((2 * s + core) * R, R), R)

    def chunk(q):
        return pl.ds(pl.multiple_of(q * CH, CH), CH)

    def tile(j):
        return pl.ds(pl.multiple_of(j * T, T), T)

    def remote(src, dst, send, recv, to):
        return pltpu.make_async_remote_copy(
            src_ref=src, dst_ref=dst, send_sem=send, recv_sem=recv,
            device_id={"tp": to}, device_id_type=pl.DeviceIdType.MESH,
        )

    def line(way, hop, s, q, own=False):
        here = dy_all.at[rows(s, c), chunk(q)]
        src = dy.at[:, chunk(q)] if own else here
        return remote(src, here, ls.at[way, hop, q], lr.at[s, q], t + 2 - 4 * way)

    def across(s, q, own=False):
        here = dy_all.at[rows(s, c), chunk(q)]
        src = dy.at[:, chunk(q)] if own else here
        return remote(src, here, ps.at[s, q], pr.at[s, q], partner)

    def gather_step(k, q):
        hop = k + 1

        @pl.when(z >= hop)
        def _():
            line(0, hop, z - hop, q).wait_recv()

            @pl.when(z < 3)
            def _():
                line(0, hop, z - hop, q).start()

            across(z - hop, q).start()

        @pl.when(z + hop <= 3)
        def _():
            line(1, hop, z + hop, q).wait_recv()

            @pl.when(z > 0)
            def _():
                line(1, hop, z + hop, q).start()

            across(z + hop, q).start()

    def pair(k, g):
        return remote(
            psend.at[:, chunk(g)], precv.at[k % 2, :, chunk(g)], pss.at[g], psr.at[k % 2, g], partner
        )

    def chain(way, a, g):
        return remote(
            cs.at[way, :, chunk(g)], crecv.at[way, (a - 1) % 2, :, chunk(g)],
            css.at[way, g], csr.at[way, (a - 1) % 2, g], t + 2 - 4 * way,
        )

    def strips(step):
        @pl.loop(0, R // STRIP)
        def _(i):
            step(pl.ds(pl.multiple_of(i * STRIP, STRIP), STRIP))

    def pair_add(k, s, g):
        pair(k, g).wait_recv()
        source = jnp.logical_and(z % 3 == 0, k > 0)
        way = z // 3

        @pl.when(source)
        def _():
            @pl.when(k >= 2)
            def _():
                chain(way, k, g).wait_send()

            @pl.when(jnp.logical_and(k == 3, g == 0))
            def _():
                pl.semaphore_wait(credit, 1)

            def step(r):
                total = held[s, r, chunk(g)] + precv[k % 2, r, chunk(g)].astype(F32)
                cs[way, r, chunk(g)] = total.astype(BF16)

            strips(step)
            chain(way, k, g).start()

        @pl.when(jnp.logical_not(source))
        def _():
            def step(r):
                held[s, r, chunk(g)] += precv[k % 2, r, chunk(g)].astype(F32)

            strips(step)

    def arrive(way, a, g, forward, sent_before):
        d = a + way * (3 - 2 * a)
        chain(way, a, g).wait_recv()
        old = (a - 1) % 2

        @pl.when(forward)
        def _():
            @pl.when(sent_before)
            def _():
                chain(way, a, g).wait_send()

            def step(r):
                total = held[d, r, chunk(g)] + crecv[way, old, r, chunk(g)].astype(F32)
                cs[way, r, chunk(g)] = total.astype(BF16)

            strips(step)
            chain(way, a, g).start()

        @pl.when(jnp.logical_not(forward))
        def _():
            def step(r):
                held[d, r, chunk(g)] += crecv[way, old, r, chunk(g)].astype(F32)

            strips(step)

    middle = jnp.logical_and(z >= 1, z <= 2)

    H = T // 2

    def load(src, lo, n, slot, part):
        return pltpu.make_async_copy(
            src, ring.at[slot, pl.ds(part * H, H), :], ws.at[slot, part]
        )

    def fetch(n):
        i, slot = n % 28, n % SLOTS

        @pl.when(n < 112)
        def _():
            for part in range(2):

                @pl.when(i < 14)
                def _():
                    src = w_down.at[
                        pl.ds(pl.multiple_of((i // 2) * T + part * H, H), H),
                        pl.ds(pl.multiple_of((i % 2) * F, F), F),
                    ]
                    load(src, 0, n, slot, part).start()

                @pl.when(i >= 14)
                def _():
                    src = w_in.at[pl.ds(pl.multiple_of((i - 14) * T + part * H, H), H), :]
                    load(src, 0, n, slot, part).start()

    def ready(n):
        slot = n % SLOTS
        for part in range(2):
            load(w_in.at[pl.ds(0, H), :], 0, n, slot, part).wait()
        return slot

    def pre_copies(s, m):
        return [
            pltpu.make_async_copy(
                pre.at[rows(s, core), tile(m)], preb.at[m % 2, pl.ds(i * R, R), :], prs.at[m % 2, i]
            )
            for i, core in enumerate((c, 1 - c))
        ]

    def out_copies(s):
        return [
            pltpu.make_async_copy(v.at[pl.ds(i * R, R), :], o.at[rows(s, core), :], ios.at[2 + 2 * j + i])
            for j, (v, o) in enumerate(((dpre, d_pre), (hid, hidden)))
            for i, core in enumerate((c, 1 - c))
        ]

    barrier = pltpu.get_barrier_semaphore()
    pl.semaphore_signal(barrier, inc=1, device_id={"tp": partner}, device_id_type=pl.DeviceIdType.MESH)

    @pl.when(z > 0)
    def _():
        pl.semaphore_signal(barrier, inc=1, device_id={"tp": t - 2}, device_id_type=pl.DeviceIdType.MESH)

    @pl.when(z < 3)
    def _():
        pl.semaphore_signal(barrier, inc=1, device_id={"tp": t + 2}, device_id_type=pl.DeviceIdType.MESH)

    for n in range(SLOTS - 1):
        fetch(jnp.int32(n))

    @pl.when(middle)
    def _():
        pl.semaphore_wait(barrier, 3)

    @pl.when(jnp.logical_not(middle))
    def _():
        pl.semaphore_wait(barrier, 2)

    @pl.loop(0, G)
    def _(q):
        @pl.when(z < 3)
        def _():
            line(0, 0, z, q, own=True).start()

        @pl.when(z > 0)
        def _():
            line(1, 0, z, q, own=True).start()

        across(z, q, own=True).start()

    mirror = z // 2
    u = z + mirror * (3 - 2 * z)

    @pl.loop(0, 4)
    def _(k):
        base = (k // 2) * k + (1 - k // 2) * ((k + u) % 2)
        s = base + mirror * (3 - 2 * base)

        for cp in pre_copies(s, 0):
            cp.start()

        @pl.when(k == 0)
        def _():
            pltpu.make_async_copy(dy, dyv.at[pl.ds(0, R), :], ios.at[0]).start()

        @pl.when(k > 0)
        def _():
            pltpu.make_async_copy(dy_all.at[rows(s, c), :], dyv.at[pl.ds(0, R), :], ios.at[0]).start()

        @pl.loop(0, G)
        def _(q):
            across(s, q).wait_recv()

        other = pltpu.make_async_copy(dy_all.at[rows(s, 1 - c), :], dyv.at[pl.ds(R, R), :], ios.at[1])
        other.start()
        pltpu.make_async_copy(dy, dyv.at[pl.ds(0, R), :], ios.at[0]).wait()

        keep = pltpu.make_async_copy(dyv.at[pl.ds(0, R), :], dy_all.at[rows(s, c), :], ios.at[0])

        @pl.when(k == 0)
        def _():
            keep.start()

        other.wait()

        @pl.loop(0, G)
        def _(m):
            n = 28 * k + 2 * m
            fetch(n + SLOTS - 1)
            slot = ready(n)
            acc[...] = lax.dot_general(dyv[:, :F], ring[slot], NT, preferred_element_type=F32)
            fetch(n + SLOTS)
            slot = ready(n + 1)
            acc[...] += lax.dot_general(dyv[:, F:], ring[slot], NT, preferred_element_type=F32)

            @pl.when(m < G - 1)
            def _():
                for cp in pre_copies(s, m + 1):
                    cp.start()

            for cp in pre_copies(s, m):
                cp.wait()

            @pl.loop(0, 2 * R // STRIP)
            def _(i):
                strip = pl.ds(pl.multiple_of(i * STRIP, STRIP), STRIP)
                v = preb[m % 2, strip, :].astype(F32)
                sq = v * v
                th = jnp.tanh((C0 * v) * (1.0 + C1 * sq))
                cdf = 0.5 + 0.5 * th
                slope = cdf + (v * (1.0 - th * th)) * (0.5 * C0) * (1.0 + (3 * C1) * sq)
                dpre[strip, tile(m)] = (acc[strip, :] * slope).astype(BF16)
                hid[strip, tile(m)] = (v * cdf).astype(BF16)

            @pl.when(jnp.logical_and(k < 3, m % 2 == 1))
            def _():
                gather_step(k, m // 2)

            @pl.when(jnp.logical_and(k >= 2, middle))
            def _():
                arrive(z - 1, k - 1, m, k == 3, False)

        @pl.when(jnp.logical_and(k == 2, middle))
        def _():
            pl.semaphore_signal(
                credit, inc=1, device_id={"tp": t - 2 + 4 * (z - 1)}, device_id_type=pl.DeviceIdType.MESH
            )

        @pl.when(k == 0)
        def _():
            keep.wait()

        for cp in out_copies(s):
            cp.start()

        @pl.loop(0, G)
        def _(m):
            for half in range(2):
                n = 28 * k + 14 + 2 * m + half
                fetch(n + SLOTS - 1)
                slot = ready(n)
                term = lax.dot_general(dpre[...], ring[slot], NT, preferred_element_type=F32)
                held[s, :, tile(2 * m + half)] = term[:R]
                psend[:, tile(2 * m + half)] = term[R:].astype(BF16)
            pair(k, m).start()

            @pl.when(jnp.logical_and(k < 3, m % 2 == 0))
            def _():
                gather_step(k, 3 + m // 2)

            @pl.when(jnp.logical_and(k == 3, middle))
            def _():
                arrive(2 - z, 2, m, False, False)

            @pl.when(m > 0)
            def _():
                pair_add(k, s, m - 1)

        pair_add(k, s, G - 1)

        @pl.loop(0, G)
        def _(m):
            pair(k, m).wait_send()

        for cp in out_copies(s):
            cp.wait()

    @pl.loop(0, G + 1)
    def _(g):
        @pl.when(jnp.logical_and(g < G, middle))
        def _():
            arrive(z - 1, 3, g, True, True)

        @pl.when(jnp.logical_and(g > 0, middle))
        def _():
            arrive(2 - z, 3, g - 1, True, False)

        @pl.when(jnp.logical_and(g < G, jnp.logical_not(middle)))
        def _():
            arrive((3 - z) // 3, 3, g, False, False)

    @pl.loop(0, G)
    def _(g):
        def step(r):
            psend[r, chunk(g)] = held[z, r, chunk(g)].astype(BF16)

        strips(step)

    out = pltpu.make_async_copy(psend, dx, ios.at[0])
    out.start()

    @pl.loop(0, G)
    def _(q):
        @pl.when(middle)
        def _():
            chain(0, 3, q).wait_send()
            chain(1, 3, q).wait_send()

        @pl.when(jnp.logical_not(middle))
        def _():
            chain(z // 3, 3, q).wait_send()

        for hop in range(3):

            @pl.when(jnp.logical_and(z >= hop, z < 3))
            def _():
                line(0, hop, z, q).wait_send()

            @pl.when(jnp.logical_and(z + hop <= 3, z > 0))
            def _():
                line(1, hop, z, q).wait_send()

        for s in range(4):
            across(s, q).wait_send()

    out.wait()


def gather_reduce(dy, pre, w_in, w_down):
    R, D = dy.shape
    rows, F = pre.shape
    T = F // G
    dma = pltpu.SemaphoreType.DMA
    any_spec = pl.BlockSpec(memory_space=pl.ANY)
    return pl.pallas_call(
        gather_reduce_kernel,
        name="gather_reduce",
        out_shape=(
            jax.ShapeDtypeStruct((rows, D), BF16),
            jax.ShapeDtypeStruct((rows, F), BF16),
            jax.ShapeDtypeStruct((rows, F), BF16),
            jax.ShapeDtypeStruct((R, D), BF16),
        ),
        in_specs=[any_spec] * 4,
        out_specs=[any_spec] * 4,
        scratch_shapes=[
            pltpu.VMEM((2 * R, D), BF16),
            pltpu.VMEM((SLOTS, T, F), BF16),
            pltpu.VMEM((2 * R, F), BF16),
            pltpu.VMEM((2 * R, F), BF16),
            pltpu.VMEM((2, 2 * R, T), BF16),
            pltpu.VMEM((4, R, D), F32),
            pltpu.VMEM((2, R, D), BF16),
            pltpu.VMEM((R, D), BF16),
            pltpu.VMEM((2, 2, R, D), BF16),
            pltpu.VMEM((2, R, D), BF16),
            pltpu.VMEM((2 * R, T), F32),
            dma((SLOTS, 2)),
            dma((6,)),
            dma((2, 2)),
            dma((2, 3, G)),
            dma((4, G)),
            dma((4, G)),
            dma((4, G)),
            dma((G,)),
            dma((2, G)),
            dma((2, G)),
            dma((2, 2, G)),
            pltpu.SemaphoreType.REGULAR,
        ],
        compiler_params=pltpu.CompilerParams(
            collective_id=0, has_side_effects=True, vmem_limit_bytes=VMEM
        ),
        cost_estimate=pl.CostEstimate(
            flops=4 * rows * D * F, bytes_accessed=16 * D * F, transcendentals=rows * F
        ),
    )(dy, pre, w_in, w_down)


def weight_grad_kernel(a, b, *rest):
    o = rest[-1]
    o[...] = lax.dot_general(a[...], b[...], TN, preferred_element_type=F32).astype(BF16)


def weight_grad(a, b, total, start, into, bm, bn):
    rows, A = a.shape
    B = b.shape[1]
    off = start // bm
    return pl.pallas_call(
        weight_grad_kernel,
        name="weight_grad",
        grid=(B // bn, A // bm),
        out_shape=jax.ShapeDtypeStruct((total, B), BF16),
        in_specs=[
            pl.BlockSpec((rows, bm), lambda j, i: (0, i)),
            pl.BlockSpec((rows, bn), lambda j, i: (0, j)),
        ]
        + ([] if into is None else [pl.BlockSpec(memory_space=pl.ANY)]),
        out_specs=pl.BlockSpec((bm, bn), lambda j, i: (i + off, j)),
        input_output_aliases={} if into is None else {2: 0},
        compiler_params=pltpu.CompilerParams(
            dimension_semantics=("arbitrary", "arbitrary"), vmem_limit_bytes=VMEM
        ),
        cost_estimate=pl.CostEstimate(
            flops=2 * rows * A * B, bytes_accessed=2 * (rows * (A + B) + A * B), transcendentals=0
        ),
    )(a, b, *([] if into is None else [into]))


CUTS = (0, 2304, 4608, 7168)


def solution(mesh):
    def body(x, dy, pre, w_in, w_down):
        dy_all, d_pre, hidden, dx = gather_reduce(dy, pre, w_in, w_down)
        x_late, d_pre = lax.optimization_barrier((x, d_pre))
        D, F = w_in.shape
        dw_down = weight_grad(hidden, dy_all, F, 0, None, 896, 1792)
        dw_in = None
        for lo, hi in zip(CUTS[:-1], CUTS[1:]):
            piece = lax.all_gather(x_late[:, lo:hi], "tp", axis=0, tiled=True)
            dw_in = weight_grad(piece, d_pre, D, lo, dw_in, 256, 3584)
        return dx, dw_in, dw_down

    rows = P(("dp", "tp"), None)
    return jax.shard_map(
        body,
        mesh=mesh,
        in_specs=(rows, rows, P("dp", "tp"), P(None, "tp"), P("tp", None)),
        out_specs=(rows, P("dp", "tp"), P(("dp", "tp"), None)),
        check_vma=False,
    )
```

```python
import functools

import jax
import jax.numpy as jnp
from jax import lax
from jax.experimental import pallas as pl
from jax.experimental.pallas import tpu as pltpu
from jax.sharding import PartitionSpec as P

F32, BF16 = jnp.float32, jnp.bfloat16
NT = (((1,), (1,)), ((), ()))
TN = (((0,), (0,)), ((), ()))
G = 7
STRIP = 16
SLOTS = 5
VMEM = 67043328
XG = 4
GC = 14
XL = 2560
XW = 2048
C0 = 0.7978845608028654
C1 = 0.044715


def gather_reduce_kernel(
    x, dy, pre, w_in, w_down, dy_all, d_pre, hidden, dx, x_part, slopes, x_late0, x_late1,
    dyv, ring, dpre, slp, held, precv, psend, crecv, cs,
    acc, ws, ios, els, prs, ls, lr, ps, pr, xls, xlr, xps, xpr, pss, psr, css, csr, credit,
):
    R, D = dy.shape
    F = pre.shape[1]
    CH, T = D // G, F // G
    XC = x_part.shape[1] // XG
    t = lax.axis_index("tp")
    z, c = t // 2, t % 2
    partner = t + 1 - 2 * c

    def rows(s, core):
        return pl.ds(pl.multiple_of((2 * s + core) * R, R), R)

    def chunk(q):
        return pl.ds(pl.multiple_of(q * CH, CH), CH)

    def slab(q):
        return pl.ds(pl.multiple_of(q * (D // GC), D // GC), D // GC)

    def tile(j):
        return pl.ds(pl.multiple_of(j * T, T), T)

    def remote(src, dst, send, recv, to):
        return pltpu.make_async_remote_copy(
            src_ref=src, dst_ref=dst, send_sem=send, recv_sem=recv,
            device_id={"tp": to}, device_id_type=pl.DeviceIdType.MESH,
        )

    def line(way, hop, s, q, own=False):
        here = dy_all.at[rows(s, c), chunk(q)]
        src = dy.at[:, chunk(q)] if own else here
        return remote(src, here, ls.at[way, hop, q], lr.at[s, q], t + 2 - 4 * way)

    def across(s, q, own=False):
        here = dy_all.at[rows(s, c), chunk(q)]
        src = dy.at[:, chunk(q)] if own else here
        return remote(src, here, ps.at[s, q], pr.at[s, q], partner)

    def xcols(q):
        return pl.ds(pl.multiple_of(q * XC, XC), XC)

    def x_line(way, hop, s, q, own=False):
        here = x_part.at[rows(s, c), xcols(q)]
        src = x.at[:, xcols(q)] if own else here
        return remote(src, here, xls.at[way, hop, q], xlr.at[s, q], t + 2 - 4 * way)

    def x_across(s, q, own=False):
        here = x_part.at[rows(s, c), xcols(q)]
        src = x.at[:, xcols(q)] if own else here
        return remote(src, here, xps.at[s, q], xpr.at[s, q], partner)

    def send_own(along, over, q):
        @pl.when(z < 3)
        def _():
            along(0, 0, z, q, own=True).start()

        @pl.when(z > 0)
        def _():
            along(1, 0, z, q, own=True).start()

        over(z, q, own=True).start()

    def pass_on(along, over, hop, q):
        @pl.when(z >= hop)
        def _():
            along(0, hop, z - hop, q).wait_recv()

            @pl.when(z < 3)
            def _():
                along(0, hop, z - hop, q).start()

            over(z - hop, q).start()

        @pl.when(z + hop <= 3)
        def _():
            along(1, hop, z + hop, q).wait_recv()

            @pl.when(z > 0)
            def _():
                along(1, hop, z + hop, q).start()

            over(z + hop, q).start()

    def drain(along, over, q):
        for hop in range(3):

            @pl.when(jnp.logical_and(z >= hop, z < 3))
            def _():
                along(0, hop, z, q).wait_send()

            @pl.when(jnp.logical_and(z + hop <= 3, z > 0))
            def _():
                along(1, hop, z, q).wait_send()

        for s in range(4):
            over(s, q).wait_send()

    def pair(k, g):
        return remote(
            psend.at[:, chunk(g)], precv.at[k % 2, :, chunk(g)], pss.at[g], psr.at[k % 2, g], partner
        )

    def chain(way, a, g):
        return remote(
            cs.at[way, :, slab(g)], crecv.at[way, (a - 1) % 2, :, slab(g)],
            css.at[way, g], csr.at[way, (a - 1) % 2, g], t + 2 - 4 * way,
        )

    def strips(step):
        @pl.loop(0, R // STRIP)
        def _(i):
            step(pl.ds(pl.multiple_of(i * STRIP, STRIP), STRIP))

    def pair_add(k, s, g):
        pair(k, g).wait_recv()
        source = jnp.logical_and(z % 3 == 0, k < 3)
        way = z // 3

        @pl.when(source)
        def _():
            @pl.when(jnp.logical_and(k == 2, g == 0))
            def _():
                pl.semaphore_wait(credit, 1)

            @pl.loop(0, GC // G)
            def _(j):
                piece = g * (GC // G) + j

                @pl.when(k >= 1)
                def _():
                    chain(way, k + 1, piece).wait_send()

                def step(r):
                    total = held[s, r, slab(piece)] + precv[k % 2, r, slab(piece)].astype(F32)
                    cs[way, r, slab(piece)] = total.astype(BF16)

                strips(step)
                chain(way, k + 1, piece).start()

        @pl.when(jnp.logical_not(source))
        def _():
            def step(r):
                held[s, r, chunk(g)] += precv[k % 2, r, chunk(g)].astype(F32)

            strips(step)

    def arrive(way, a, g, forward, sent_before):
        d = a + way * (3 - 2 * a)
        chain(way, a, g).wait_recv()
        old = (a - 1) % 2

        @pl.when(forward)
        def _():
            @pl.when(sent_before)
            def _():
                chain(way, a, g).wait_send()

            def step(r):
                total = held[d, r, slab(g)] + crecv[way, old, r, slab(g)].astype(F32)
                cs[way, r, slab(g)] = total.astype(BF16)

            strips(step)
            chain(way, a, g).start()

        @pl.when(jnp.logical_not(forward))
        def _():
            def step(r):
                held[d, r, slab(g)] += crecv[way, old, r, slab(g)].astype(F32)

            strips(step)

    middle = jnp.logical_and(z >= 1, z <= 2)
    ends = z % 3 == 0

    def hooks(k, v):
        @pl.when(jnp.logical_and(k >= 1, middle))
        def _():
            @pl.when(v == 0)
            def _():
                @pl.loop(0, 3)
                def _(g):
                    arrive(z - 1, k, g, k > 1, k == 3)

            @pl.when(v <= 10)
            def _():
                arrive(z - 1, k, v + 3, k > 1, k == 3)

        @pl.when(jnp.logical_and(k == 3, middle))
        def _():
            @pl.when(v < G)
            def _():
                @pl.loop(0, 2)
                def _(j):
                    arrive(2 - z, 2, 2 * v + j, False, False)

            @pl.when(v >= 3)
            def _():
                arrive(2 - z, 3, v - 3, True, False)

    def late(k):
        @pl.when(jnp.logical_and(k == 3, middle))
        def _():
            @pl.loop(GC - 3, GC)
            def _(g):
                arrive(2 - z, 3, g, True, False)

    H = T // 2

    def load(src, lo, n, slot, part):
        return pltpu.make_async_copy(
            src, ring.at[slot, pl.ds(part * H, H), :], ws.at[slot, part]
        )

    def fetch(n):
        i, slot = n % 28, n % SLOTS

        @pl.when(n < 112)
        def _():
            for part in range(2):

                @pl.when(i < 14)
                def _():
                    src = w_down.at[
                        pl.ds(pl.multiple_of((i // 2) * T + part * H, H), H),
                        pl.ds(pl.multiple_of((i % 2) * F, F), F),
                    ]
                    load(src, 0, n, slot, part).start()

                @pl.when(i >= 14)
                def _():
                    src = w_in.at[pl.ds(pl.multiple_of((i - 14) * T + part * H, H), H), :]
                    load(src, 0, n, slot, part).start()

    def ready(n):
        slot = n % SLOTS
        for part in range(2):
            load(w_in.at[pl.ds(0, H), :], 0, n, slot, part).wait()
        return slot

    def slope_copies(s, m):
        return [
            pltpu.make_async_copy(
                slopes.at[rows(s, core), tile(m)], slp.at[m % 2, pl.ds(i * R, R), :], prs.at[m % 2, i]
            )
            for i, core in enumerate((c, 1 - c))
        ]

    def out_copies(s):
        return [
            pltpu.make_async_copy(dpre.at[pl.ds(i * R, R), :], d_pre.at[rows(s, core), :], ios.at[2 + i])
            for i, core in enumerate((c, 1 - c))
        ]

    def e_block(i):
        return pl.ds(pl.multiple_of((i // G) * (2 * R), 2 * R), 2 * R), tile(i % G)

    def e_in(i):
        r, cl = e_block(i)
        return pltpu.make_async_copy(pre.at[r, cl], dpre.at[:, tile(i % 2)], els.at[0, i % 2])

    def e_out(i):
        r, cl = e_block(i)
        return (
            pltpu.make_async_copy(dpre.at[:, tile(2 + i % 2)], hidden.at[r, cl], els.at[1, i % 2]),
            pltpu.make_async_copy(slp.at[i % 2], slopes.at[r, cl], els.at[2, i % 2]),
        )

    def e_step(i):
        @pl.when(i + 1 < 4 * G)
        def _():
            e_in(i + 1).start()

        @pl.when(i >= 2)
        def _():
            for cp in e_out(i - 2):
                cp.wait()

        e_in(i).wait()

        @pl.loop(0, 2 * R // STRIP)
        def _(j):
            strip = pl.ds(pl.multiple_of(j * STRIP, STRIP), STRIP)
            v = dpre[strip, tile(i % 2)].astype(F32)
            sq = v * v
            th = jnp.tanh(v * (C0 + (C0 * C1) * sq))
            cdf = 0.5 + 0.5 * th
            slp[i % 2, strip, :] = cdf + (v * (1.0 - th * th)) * (0.5 * C0 + (1.5 * C0 * C1) * sq)
            dpre[strip, tile(2 + i % 2)] = (v * cdf).astype(BF16)

        for cp in e_out(i):
            cp.start()

    barrier = pltpu.get_barrier_semaphore()
    pl.semaphore_signal(barrier, inc=1, device_id={"tp": partner}, device_id_type=pl.DeviceIdType.MESH)

    @pl.when(z > 0)
    def _():
        pl.semaphore_signal(barrier, inc=1, device_id={"tp": t - 2}, device_id_type=pl.DeviceIdType.MESH)

    @pl.when(z < 3)
    def _():
        pl.semaphore_signal(barrier, inc=1, device_id={"tp": t + 2}, device_id_type=pl.DeviceIdType.MESH)

    for n in range(SLOTS):
        fetch(jnp.int32(n))

    @pl.when(middle)
    def _():
        pl.semaphore_wait(barrier, 3)

    @pl.when(jnp.logical_not(middle))
    def _():
        pl.semaphore_wait(barrier, 2)

    @pl.loop(0, G)
    def _(q):
        send_own(line, across, q)

    @pl.loop(0, 4)
    def _(s):
        def step(r):
            held[s, r, :] = jnp.zeros((STRIP, D), F32)

        strips(step)

    mine = pltpu.make_async_copy(x, dyv.at[pl.ds(0, R), :], ios.at[0])
    mine.start()
    mine.wait()
    XP, XL = x_part.shape[1], x_late0.shape[1]
    mine = [
        pltpu.make_async_copy(dyv.at[pl.ds(0, R), pl.ds(0, XP)], x_part.at[rows(z, c), :], ios.at[0]),
        pltpu.make_async_copy(dyv.at[pl.ds(0, R), pl.ds(XP, XL)], x_late0, ios.at[1]),
        pltpu.make_async_copy(dyv.at[pl.ds(0, R), pl.ds(XP + XL, XL)], x_late1, ios.at[2]),
    ]
    for cp in mine:
        cp.start()

    e_in(jnp.int32(0)).start()

    @pl.loop(0, G)
    def _(q):
        @pl.loop(0, 4)
        def _(j):
            e_step(4 * q + j)

        pass_on(line, across, 1, q)

    for i in (4 * G - 2, 4 * G - 1):
        for cp in e_out(jnp.int32(i)):
            cp.wait()
    for cp in mine:
        cp.wait()

    mirror = z // 2
    u = z + mirror * (3 - 2 * z)

    def block(k):
        base = (1 - k // 3) * (k + 1) + (k // 3) * u - ((3 - k) // 3) * u
        return base + mirror * (3 - 2 * base)

    @pl.loop(0, 4)
    def _(k):
        s = block(k)

        for cp in slope_copies(s, 0):
            cp.start()

        @pl.when(k == 3)
        def _():
            pltpu.make_async_copy(dy, dyv.at[pl.ds(0, R), :], ios.at[0]).start()

        @pl.when(k < 3)
        def _():
            pltpu.make_async_copy(dy_all.at[rows(s, c), :], dyv.at[pl.ds(0, R), :], ios.at[0]).start()

        @pl.loop(0, G)
        def _(q):
            across(s, q).wait_recv()

        other = pltpu.make_async_copy(dy_all.at[rows(s, 1 - c), :], dyv.at[pl.ds(R, R), :], ios.at[1])
        other.start()
        pltpu.make_async_copy(dy, dyv.at[pl.ds(0, R), :], ios.at[0]).wait()

        keep = pltpu.make_async_copy(dyv.at[pl.ds(0, R), :], dy_all.at[rows(s, c), :], ios.at[0])

        @pl.when(k == 3)
        def _():
            keep.start()

        other.wait()

        @pl.loop(0, G)
        def _(m):
            n = 28 * k + 2 * m
            slot = ready(n)
            acc[...] = lax.dot_general(dyv[:, :F], ring[slot], NT, preferred_element_type=F32)
            fetch(n + SLOTS)
            slot = ready(n + 1)
            for cp in slope_copies(s, m):
                cp.wait()
            d_h = acc[...] + lax.dot_general(dyv[:, F:], ring[slot], NT, preferred_element_type=F32)
            dpre[:, tile(m)] = (d_h * slp[m % 2]).astype(BF16)
            fetch(n + 1 + SLOTS)

            @pl.when(m < G - 1)
            def _():
                for cp in slope_copies(s, m + 1):
                    cp.start()

            hooks(k, m)

            @pl.when(jnp.logical_and(m == 0, k > 0))
            def _():
                pair_add(k - 1, block(k - 1), G - 1)

            @pl.when(jnp.logical_and(k < 2, m % 2 == 1))
            def _():
                pass_on(line, across, k + 2, m // 2)

            @pl.when(m < XG)
            def _():
                @pl.when(jnp.logical_or(jnp.logical_and(k == 0, ends), jnp.logical_and(k == 1, middle)))
                def _():
                    send_own(x_line, x_across, m)

                @pl.when(jnp.logical_and(k == 2, middle))
                def _():
                    pass_on(x_line, x_across, 2, m)

                @pl.when(jnp.logical_and(k == 3, ends))
                def _():
                    pass_on(x_line, x_across, 1, m)
                    pass_on(x_line, x_across, 2, m)

        @pl.when(k == 3)
        def _():
            keep.wait()

        for cp in out_copies(s):
            cp.start()

        @pl.loop(0, G)
        def _(m):
            @pl.when(k > 0)
            def _():
                pair(k - 1, m).wait_send()

            for half in range(2):
                n = 28 * k + 14 + 2 * m + half
                slot = ready(n)
                term = lax.dot_general(dpre[...], ring[slot], NT, preferred_element_type=F32)
                held[s, :, tile(2 * m + half)] += term[:R]
                psend[:, tile(2 * m + half)] = term[R:].astype(BF16)
                fetch(n + SLOTS)
            @pl.when(m > 0)
            def _():
                pair_add(k, s, m - 1)

            pair(k, m).start()

            @pl.when(jnp.logical_and(k < 2, m % 2 == 0))
            def _():
                pass_on(line, across, k + 2, 3 + m // 2)

            @pl.when(m < XG)
            def _():
                @pl.when(jnp.logical_and(k == 1, middle))
                def _():
                    pass_on(x_line, x_across, 1, m)

                @pl.when(jnp.logical_and(k == 3, ends))
                def _():
                    pass_on(x_line, x_across, 3, m)

            hooks(k, G + m)


        late(k)

        @pl.when(jnp.logical_and(k == 1, middle))
        def _():
            pl.semaphore_signal(
                credit, inc=1, device_id={"tp": t - 2 + 4 * (z - 1)}, device_id_type=pl.DeviceIdType.MESH
            )

        @pl.when(k == 3)
        def _():
            pair_add(k, s, G - 1)

        for cp in out_copies(s):
            cp.wait()

    @pl.when(ends)
    def _():
        @pl.loop(0, GC)
        def _(g):
            arrive((3 - z) // 3, 3, g, False, False)

    @pl.loop(0, G)
    def _(g):
        pair(jnp.int32(3), g).wait_send()

        def step(r):
            psend[r, chunk(g)] = held[z, r, chunk(g)].astype(BF16)

        strips(step)

    out = pltpu.make_async_copy(psend, dx, ios.at[0])
    out.start()

    @pl.loop(0, GC)
    def _(q):
        @pl.when(middle)
        def _():
            chain(0, 3, q).wait_send()
            chain(1, 3, q).wait_send()

        @pl.when(jnp.logical_not(middle))
        def _():
            chain(z // 3, 3, q).wait_send()

    @pl.loop(0, G)
    def _(q):
        drain(line, across, q)

    @pl.loop(0, XG)
    def _(q):
        drain(x_line, x_across, q)
        for s in range(4):
            x_across(s, q).wait_recv()

    out.wait()


def gather_reduce(x, dy, pre, w_in, w_down):
    R, D = dy.shape
    rows, F = pre.shape
    T = F // G
    dma = pltpu.SemaphoreType.DMA
    any_spec = pl.BlockSpec(memory_space=pl.ANY)
    return pl.pallas_call(
        gather_reduce_kernel,
        name="gather_reduce",
        out_shape=(
            jax.ShapeDtypeStruct((rows, D), BF16),
            jax.ShapeDtypeStruct((rows, F), BF16),
            jax.ShapeDtypeStruct((rows, F), BF16),
            jax.ShapeDtypeStruct((R, D), BF16),
            jax.ShapeDtypeStruct((rows, XW * D // 7168), BF16),
            jax.ShapeDtypeStruct((rows, F), F32),
            jax.ShapeDtypeStruct((R, D - XW * D // 7168 - XL * D // 7168), BF16),
            jax.ShapeDtypeStruct((R, XL * D // 7168), BF16),
        ),
        in_specs=[any_spec] * 5,
        out_specs=[any_spec] * 8,
        scratch_shapes=[
            pltpu.VMEM((2 * R, D), BF16),
            pltpu.VMEM((SLOTS, T, F), BF16),
            pltpu.VMEM((2 * R, F), BF16),
            pltpu.VMEM((2, 2 * R, T), F32),
            pltpu.VMEM((4, R, D), F32),
            pltpu.VMEM((2, R, D), BF16),
            pltpu.VMEM((R, D), BF16),
            pltpu.VMEM((2, 2, R, D), BF16),
            pltpu.VMEM((2, R, D), BF16),
            pltpu.VMEM((2 * R, T), F32),
            dma((SLOTS, 2)),
            dma((4,)),
            dma((3, 2)),
            dma((2, 2)),
            dma((2, 3, G)),
            dma((4, G)),
            dma((4, G)),
            dma((4, G)),
            dma((2, 3, XG)),
            dma((4, XG)),
            dma((4, XG)),
            dma((4, XG)),
            dma((G,)),
            dma((2, G)),
            dma((2, GC)),
            dma((2, 2, GC)),
            pltpu.SemaphoreType.REGULAR,
        ],
        compiler_params=pltpu.CompilerParams(
            collective_id=0, has_side_effects=True, vmem_limit_bytes=VMEM
        ),
        cost_estimate=pl.CostEstimate(
            flops=4 * rows * D * F, bytes_accessed=16 * D * F, transcendentals=rows * F
        ),
    )(x, dy, pre, w_in, w_down)


def weight_grad_kernel(a, b, *rest, copied):
    o = rest[-1]
    if copied:
        rest[-2][...] = rest[-3][...]
    o[...] = lax.dot_general(a[...], b[...], TN, preferred_element_type=F32).astype(BF16)


def weight_grad(a, b, total, start, into, bm, bn, small=None):
    rows, A = a.shape
    B = b.shape[1]
    off = start // bm
    steps = A // bm
    args = [a, b]
    in_specs = [
        pl.BlockSpec((rows, bm), lambda j, i: (0, i)),
        pl.BlockSpec((rows, bn), lambda j, i: (0, j)),
    ]
    out_shape = [jax.ShapeDtypeStruct((total, B), BF16)]
    out_specs = [pl.BlockSpec((bm, bn), lambda j, i: (i + off, j))]
    aliases = {}
    if into is not None:
        aliases = {2: 0 if small is None else 1}
        args.append(into)
        in_specs.append(pl.BlockSpec(memory_space=pl.ANY))
    if small is not None:
        spec = pl.BlockSpec((small.shape[0] // steps, small.shape[1]), lambda j, i: (i, 0))
        args.append(small)
        in_specs.append(spec)
        out_shape.insert(0, jax.ShapeDtypeStruct(small.shape, BF16))
        out_specs.insert(0, spec)
    out = pl.pallas_call(
        functools.partial(weight_grad_kernel, copied=small is not None),
        name="weight_grad",
        grid=(B // bn, steps),
        out_shape=out_shape,
        in_specs=in_specs,
        out_specs=out_specs,
        input_output_aliases=aliases,
        compiler_params=pltpu.CompilerParams(
            dimension_semantics=("arbitrary", "arbitrary"), vmem_limit_bytes=VMEM
        ),
        cost_estimate=pl.CostEstimate(
            flops=2 * rows * A * B, bytes_accessed=2 * (rows * (A + B) + A * B), transcendentals=0
        ),
    )(*args)
    return out[0] if small is None else out


WITH_X, NOUT = True, 8


def solution(mesh):
    def body(x, dy, pre, w_in, w_down):
        dy_all, d_pre, hidden, dx, x_part, _, *late = gather_reduce(x, dy, pre, w_in, w_down)
        late = [lax.all_gather(piece, "tp", axis=0, tiled=True) for piece in late]
        D, F = w_in.shape
        dw_in = weight_grad(x_part, d_pre, D, 0, None, 1024, 1792)
        dw_down = weight_grad(hidden, dy_all, F, 0, None, 896, 1792)
        dw_in = weight_grad(late[0], d_pre, D, XW, dw_in, 512, 3584)
        dx, dw_in = weight_grad(late[1], d_pre, D, XW + XL, dw_in, 512, 3584, small=dx)
        return dx, dw_in, dw_down

    rows = P(("dp", "tp"), None)
    return jax.shard_map(
        body,
        mesh=mesh,
        in_specs=(rows, rows, P("dp", "tp"), P(None, "tp"), P("tp", None)),
        out_specs=(rows, P("dp", "tp"), P(("dp", "tp"), None)),
        check_vma=False,
    )
```

```python
import functools

import jax
import jax.numpy as jnp
from jax import lax
from jax.experimental import pallas as pl
from jax.experimental.pallas import tpu as pltpu
from jax.sharding import PartitionSpec as P

F32, BF16 = jnp.float32, jnp.bfloat16
NT = (((1,), (1,)), ((), ()))
TN = (((0,), (0,)), ((), ()))
G = 7
STRIP = 16
SLOTS = 4
VMEM = 67043328
XG = 9
GC = 14
BI, BJ = 4, 4
XG = 9
GC = 14
XL = 2560
NB = 5
XW = 4608
XL = 2048
C0 = 0.7978845608028654
C1 = 0.044715


def gather_reduce_kernel(
    x, dy, pre, w_in, w_down, dy_all, d_pre, hidden, dx, x_part, x_late0, x_late1, down,
    held, precv, psend, crecv, cs,
    ws, ios, hos, prs, ls, lr, ps, pr, xls, xlr, xps, xpr, pss, psr, css, csr, fas, fbs, fos, credit,
):
    R, D = dy.shape
    F = pre.shape[1]
    CH, T = D // G, F // G
    XC = x_part.shape[1] // XG
    t = lax.axis_index("tp")
    z, c = t // 2, t % 2
    partner = t + 1 - 2 * c

    def rows(s, core):
        return pl.ds(pl.multiple_of((2 * s + core) * R, R), R)

    def chunk(q):
        return pl.ds(pl.multiple_of(q * CH, CH), CH)

    def slab(q):
        return pl.ds(pl.multiple_of(q * (D // GC), D // GC), D // GC)

    def tile(j):
        return pl.ds(pl.multiple_of(j * T, T), T)

    def remote(src, dst, send, recv, to):
        return pltpu.make_async_remote_copy(
            src_ref=src, dst_ref=dst, send_sem=send, recv_sem=recv,
            device_id={"tp": to}, device_id_type=pl.DeviceIdType.MESH,
        )

    def line(way, hop, s, q, own=False):
        here = dy_all.at[rows(s, c), chunk(q)]
        src = dy.at[:, chunk(q)] if own else here
        return remote(src, here, ls.at[way, hop, q], lr.at[s, q], t + 2 - 4 * way)

    def across(s, q, own=False):
        here = dy_all.at[rows(s, c), chunk(q)]
        src = dy.at[:, chunk(q)] if own else here
        return remote(src, here, ps.at[s, q], pr.at[s, q], partner)

    def xcols(q):
        return pl.ds(pl.multiple_of(q * XC, XC), XC)

    def x_line(way, hop, s, q, own=False):
        here = x_part.at[rows(s, c), xcols(q)]
        src = x.at[:, xcols(q)] if own else here
        return remote(src, here, xls.at[way, hop, q], xlr.at[s, q], t + 2 - 4 * way)

    def x_across(s, q, own=False):
        here = x_part.at[rows(s, c), xcols(q)]
        src = x.at[:, xcols(q)] if own else here
        return remote(src, here, xps.at[s, q], xpr.at[s, q], partner)

    def send_own(along, over, q):
        over(z, q, own=True).start()

        @pl.when(z < 3)
        def _():
            along(0, 0, z, q, own=True).start()

        @pl.when(z > 0)
        def _():
            along(1, 0, z, q, own=True).start()

    def pass_on(along, over, hop, q):
        @pl.when(z >= hop)
        def _():
            along(0, hop, z - hop, q).wait_recv()

            @pl.when(z < 3)
            def _():
                along(0, hop, z - hop, q).start()

            over(z - hop, q).start()

        @pl.when(z + hop <= 3)
        def _():
            along(1, hop, z + hop, q).wait_recv()

            @pl.when(z > 0)
            def _():
                along(1, hop, z + hop, q).start()

            over(z + hop, q).start()

    def drain(along, over, q):
        for hop in range(3):

            @pl.when(jnp.logical_and(z >= hop, z < 3))
            def _():
                along(0, hop, z, q).wait_send()

            @pl.when(jnp.logical_and(z + hop <= 3, z > 0))
            def _():
                along(1, hop, z, q).wait_send()

        for s in range(4):
            over(s, q).wait_send()

    def pair(k, g):
        return remote(
            psend.at[:, chunk(g)], precv.at[:, chunk(g)], pss.at[g], psr.at[g], partner
        )

    def chain(way, a, g):
        return remote(
            cs.at[way, :, slab(g)], crecv.at[way, (a - 1) % 2, :, slab(g)],
            css.at[way, g], csr.at[way, (a - 1) % 2, g], t + 2 - 4 * way,
        )

    def strips(step):
        @pl.loop(0, R // STRIP)
        def _(i):
            step(pl.ds(pl.multiple_of(i * STRIP, STRIP), STRIP))

    def pair_add(k, s, g):
        pair(k, g).wait_recv()
        source = jnp.logical_and(z % 3 == 0, k > 0)
        way = z // 3

        @pl.when(source)
        def _():
            @pl.when(jnp.logical_and(k == 3, g == 0))
            def _():
                pl.semaphore_wait(credit, 1)

            @pl.loop(0, GC // G)
            def _(j):
                piece = g * (GC // G) + j

                @pl.when(k >= 2)
                def _():
                    chain(way, k, piece).wait_send()

                def step(r):
                    total = held[s, r, slab(piece)] + precv[r, slab(piece)].astype(F32)
                    cs[way, r, slab(piece)] = total.astype(BF16)

                strips(step)
                chain(way, k, piece).start()

        @pl.when(jnp.logical_not(source))
        def _():
            def step(r):
                held[s, r, chunk(g)] += precv[r, chunk(g)].astype(F32)

            strips(step)

    def arrive(way, a, g, forward, sent_before):
        d = a + way * (3 - 2 * a)
        chain(way, a, g).wait_recv()
        old = (a - 1) % 2

        @pl.when(forward)
        def _():
            @pl.when(sent_before)
            def _():
                chain(way, a, g).wait_send()

            def step(r):
                total = held[d, r, slab(g)] + crecv[way, old, r, slab(g)].astype(F32)
                cs[way, r, slab(g)] = total.astype(BF16)

            strips(step)
            chain(way, a, g).start()

        @pl.when(jnp.logical_not(forward))
        def _():
            def step(r):
                held[d, r, slab(g)] += crecv[way, old, r, slab(g)].astype(F32)

            strips(step)

    middle = jnp.logical_and(z >= 1, z <= 2)
    ends = z % 3 == 0

    def hooks(k, v):
        @pl.when(jnp.logical_and(k < 3, v % 2 == 1))
        def _():
            pass_on(line, across, k + 1, v // 2)

        def x_pair(v, step):
            for j in range(2):

                @pl.when(jnp.logical_and(v >= 0, 2 * v + j < XG))
                def _():
                    step(2 * v + j)

        @pl.when(jnp.logical_or(jnp.logical_and(k == 1, ends), jnp.logical_and(k == 2, middle)))
        def _():
            x_pair(v, lambda q: send_own(x_line, x_across, q))

        @pl.when(jnp.logical_and(k == 2, middle))
        def _():
            x_pair(v - G, lambda q: pass_on(x_line, x_across, 1, q))

        @pl.when(jnp.logical_and(k == 3, middle))
        def _():
            x_pair(v, lambda q: pass_on(x_line, x_across, 2, q))

        @pl.when(jnp.logical_and(k >= 2, middle))
        def _():
            @pl.when(v == 0)
            def _():
                @pl.loop(0, 3)
                def _(g):
                    arrive(z - 1, k - 1, g, k == 3, False)

            @pl.when(v <= 10)
            def _():
                arrive(z - 1, k - 1, v + 3, k == 3, False)

    def tail_hooks(f):
        def sums(j, way, a, forward, sent_before):
            @pl.loop(0, 2)
            def _(i):
                arrive(way, a, 2 * j + i, forward, sent_before)

        @pl.when(middle)
        def _():
            @pl.when(f < 7)
            def _():
                sums(f, z - 1, 3, True, True)

            @pl.when(jnp.logical_and(jnp.logical_and(f >= 3, f <= 12), f % 3 < 2))
            def _():
                sums(2 * (f // 3 - 1) + f % 3, 2 - z, 3, True, False)

            @pl.when(jnp.logical_and(jnp.logical_and(f >= 5, f <= 11), f % 3 == 2))
            def _():
                @pl.loop(0, 5)
                def _(i):
                    g = 5 * (f // 3 - 1) + i

                    @pl.when(g < GC)
                    def _():
                        arrive(2 - z, 2, g, False, False)

        @pl.when(ends)
        def _():
            def x_four(f, hop):
                for j in range(4):

                    @pl.when(4 * f + j < XG)
                    def _():
                        pass_on(x_line, x_across, hop, 4 * f + j)

            @pl.when(f < 3)
            def _():
                x_four(f, 1)

            @pl.when(jnp.logical_and(f >= 3, f < 6))
            def _():
                x_four(f - 3, 2)

            @pl.when(jnp.logical_and(f >= 9, f < 12))
            def _():
                x_four(f - 9, 3)

            @pl.when(jnp.logical_and(jnp.logical_and(f >= 8, f <= 15), f % 3 != 1))
            def _():
                sums(2 * ((f - 8) // 3) + (f - 8) % 3, (3 - z) // 3, 3, False, False)

    barrier = pltpu.get_barrier_semaphore()
    pl.semaphore_signal(barrier, inc=1, device_id={"tp": partner}, device_id_type=pl.DeviceIdType.MESH)

    @pl.when(z > 0)
    def _():
        pl.semaphore_signal(barrier, inc=1, device_id={"tp": t - 2}, device_id_type=pl.DeviceIdType.MESH)

    @pl.when(z < 3)
    def _():
        pl.semaphore_signal(barrier, inc=1, device_id={"tp": t + 2}, device_id_type=pl.DeviceIdType.MESH)


    @pl.when(middle)
    def _():
        pl.semaphore_wait(barrier, 3)

    @pl.when(jnp.logical_not(middle))
    def _():
        pl.semaphore_wait(barrier, 2)

    @pl.loop(0, G)
    def _(q):
        send_own(line, across, q)

    stage = pltpu.make_async_copy(x, psend, fos.at[0])
    stage.start()
    XP, XA = x_part.shape[1], x_late0.shape[1]
    staged = [
        pltpu.make_async_copy(psend.at[:, pl.ds(0, XP)], x_part.at[rows(z, c), :], fos.at[0]),
        pltpu.make_async_copy(psend.at[:, pl.ds(XP, XA)], x_late0, fos.at[1]),
        pltpu.make_async_copy(psend.at[:, pl.ds(XP + XA, D - XP - XA)], x_late1, fas.at[0]),
    ]

    mirror = z // 2
    u = z + mirror * (3 - 2 * z)

    def block(k):
        base = (k // 2) * k + (1 - k // 2) * ((k + u) % 2)
        return base + mirror * (3 - 2 * base)

    def passes(dyv, ring, dpre, hid, preb, acc):
        H = T // 2

        def load(src, lo, n, slot, part):
            return pltpu.make_async_copy(
                src, ring.at[slot, pl.ds(part * H, H), :], ws.at[slot, part]
            )

        def fetch(n):
            i, slot = n % 28, n % SLOTS

            @pl.when(n < 112)
            def _():
                for part in range(2):

                    @pl.when(i < 14)
                    def _():
                        src = w_down.at[
                            pl.ds(pl.multiple_of((i // 2) * T + part * H, H), H),
                            pl.ds(pl.multiple_of((i % 2) * F, F), F),
                        ]
                        load(src, 0, n, slot, part).start()

                    @pl.when(i >= 14)
                    def _():
                        src = w_in.at[pl.ds(pl.multiple_of((i - 14) * T + part * H, H), H), :]
                        load(src, 0, n, slot, part).start()

        def ready(n):
            slot = n % SLOTS
            for part in range(2):
                load(w_in.at[pl.ds(0, H), :], 0, n, slot, part).wait()
            return slot

        def pre_copies(s, m):
            return [
                pltpu.make_async_copy(
                    pre.at[rows(s, core), tile(m)], preb.at[m % 2, pl.ds(i * R, R), :], prs.at[m % 2, i]
                )
                for i, core in enumerate((c, 1 - c))
            ]

        def hid_copies(s, m):
            return [
                pltpu.make_async_copy(
                    hid.at[m % 2, pl.ds(i * R, R), :], hidden.at[rows(s, core), tile(m)], hos.at[m % 2, i]
                )
                for i, core in enumerate((c, 1 - c))
            ]

        def out_copies(s):
            return [
                pltpu.make_async_copy(dpre.at[pl.ds(i * R, R), :], d_pre.at[rows(s, core), :], ios.at[2 + i])
                for i, core in enumerate((c, 1 - c))
            ]

        for n in range(SLOTS):
            fetch(jnp.int32(n))

        @pl.loop(0, 4)
        def _(k):
            s = block(k)

            for cp in pre_copies(s, 0):
                cp.start()

            @pl.when(k == 0)
            def _():
                pltpu.make_async_copy(dy, dyv.at[pl.ds(0, R), :], ios.at[0]).start()

            @pl.when(k > 0)
            def _():
                pltpu.make_async_copy(dy_all.at[rows(s, c), :], dyv.at[pl.ds(0, R), :], ios.at[0]).start()

            @pl.loop(0, G)
            def _(q):
                across(s, q).wait_recv()

            other = pltpu.make_async_copy(dy_all.at[rows(s, 1 - c), :], dyv.at[pl.ds(R, R), :], ios.at[1])
            other.start()
            pltpu.make_async_copy(dy, dyv.at[pl.ds(0, R), :], ios.at[0]).wait()

            keep = pltpu.make_async_copy(dyv.at[pl.ds(0, R), :], dy_all.at[rows(s, c), :], ios.at[0])

            @pl.when(k == 0)
            def _():
                keep.start()
                stage.wait()
                for cp in staged:
                    cp.start()

            other.wait()

            @pl.loop(0, G)
            def _(m):
                n = 28 * k + 2 * m

                @pl.when(m < G - 1)
                def _():
                    for cp in pre_copies(s, m + 1):
                        cp.start()

                slot = ready(n)
                acc[...] = lax.dot_general(dyv[:, :F], ring[slot], NT, preferred_element_type=F32)
                fetch(n + SLOTS)
                slot = ready(n + 1)
                acc[...] += lax.dot_general(dyv[:, F:], ring[slot], NT, preferred_element_type=F32)
                fetch(n + 1 + SLOTS)
                for cp in pre_copies(s, m):
                    cp.wait()

                @pl.when(m >= 2)
                def _():
                    for cp in hid_copies(s, m - 2):
                        cp.wait()

                @pl.loop(0, 2 * R // STRIP)
                def _(i):
                    strip = pl.ds(pl.multiple_of(i * STRIP, STRIP), STRIP)
                    v = preb[m % 2, strip, :].astype(F32)
                    sq = v * v
                    th = jnp.tanh(v * (C0 + (C0 * C1) * sq))
                    cdf = 0.5 + 0.5 * th
                    slope = cdf + (v * (1.0 - th * th)) * (0.5 * C0 + (1.5 * C0 * C1) * sq)
                    dpre[strip, tile(m)] = (acc[strip, :] * slope).astype(BF16)
                    hid[m % 2, strip, :] = (v * cdf).astype(BF16)

                for cp in hid_copies(s, m):
                    cp.start()

                hooks(k, m)

                @pl.when(jnp.logical_and(m == 0, k > 0))
                def _():
                    pair_add(k - 1, block(k - 1), G - 1)

            @pl.when(k == 0)
            def _():
                keep.wait()
                for cp in staged:
                    cp.wait()

            for m in (G - 2, G - 1):
                for cp in hid_copies(s, m):
                    cp.wait()

            for cp in out_copies(s):
                cp.start()

            @pl.loop(0, G)
            def _(m):
                @pl.when(k > 0)
                def _():
                    pair(k - 1, m).wait_send()

                for half in range(2):
                    n = 28 * k + 14 + 2 * m + half
                    slot = ready(n)
                    term = lax.dot_general(dpre[...], ring[slot], NT, preferred_element_type=F32)
                    held[s, :, tile(2 * m + half)] = term[:R]
                    psend[:, tile(2 * m + half)] = term[R:].astype(BF16)
                    fetch(n + SLOTS)
                @pl.when(m > 0)
                def _():
                    pair_add(k, s, m - 1)

                pair(k, m).start()

                hooks(k, G + m)


            @pl.when(jnp.logical_and(k == 2, middle))
            def _():
                pl.semaphore_signal(
                    credit, inc=1, device_id={"tp": t - 2 + 4 * (z - 1)}, device_id_type=pl.DeviceIdType.MESH
                )

            @pl.when(k == 3)
            def _():
                pair_add(k, s, G - 1)

            for cp in out_copies(s):
                cp.wait()

    pl.run_scoped(
        passes,
        pltpu.VMEM((2 * R, D), BF16),
        pltpu.VMEM((SLOTS, T, F), BF16),
        pltpu.VMEM((2 * R, F), BF16),
        pltpu.VMEM((2, 2 * R, T), BF16),
        pltpu.VMEM((2, 2 * R, T), BF16),
        pltpu.VMEM((2 * R, T), F32),
    )

    TI, TJ = F // BI, D // BJ

    def fill(fa, fb, fo):
        def strip(i, size):
            return pl.ds(pl.multiple_of(i * size, size), size)

        def a_copy(i):
            return pltpu.make_async_copy(hidden.at[:, strip(i, TI)], fa.at[i % 2], fas.at[i % 2])

        def b_copy(f):
            return pltpu.make_async_copy(dy_all.at[:, strip(f % BJ, TJ)], fb.at[f % 2], fbs.at[f % 2])

        def o_copy(f):
            return pltpu.make_async_copy(
                fo.at[f % 2], down.at[strip(f // BJ, TI), strip(f % BJ, TJ)], fos.at[f % 2]
            )

        a_copy(jnp.int32(0)).start()
        b_copy(jnp.int32(0)).start()

        @pl.loop(0, BI * BJ)
        def _(f):
            i = f // BJ

            @pl.when(f + 1 < BI * BJ)
            def _():
                b_copy(f + 1).start()

            @pl.when(f % BJ == 0)
            def _():
                @pl.when(i + 1 < BI)
                def _():
                    a_copy(i + 1).start()

                a_copy(i).wait()

            b_copy(f).wait()

            @pl.when(f >= 2)
            def _():
                o_copy(f - 2).wait()

            fo[f % 2] = lax.dot_general(
                fa[i % 2], fb[f % 2], TN, preferred_element_type=F32
            ).astype(BF16)
            o_copy(f).start()
            tail_hooks(f)

        for f in (BI * BJ - 2, BI * BJ - 1):
            o_copy(jnp.int32(f)).wait()

    pl.run_scoped(
        fill,
        pltpu.VMEM((2, 8 * R, TI), BF16),
        pltpu.VMEM((2, 8 * R, TJ), BF16),
        pltpu.VMEM((2, TI, TJ), BF16),
    )

    @pl.when(ends)
    def _():
        @pl.loop(GC - 2, GC)
        def _(g):
            arrive((3 - z) // 3, 3, g, False, False)

    @pl.loop(0, G)
    def _(g):
        pair(jnp.int32(3), g).wait_send()

        def step(r):
            psend[r, chunk(g)] = held[z, r, chunk(g)].astype(BF16)

        strips(step)

    out = pltpu.make_async_copy(psend, dx, ios.at[0])
    out.start()

    @pl.loop(0, GC)
    def _(q):
        @pl.when(middle)
        def _():
            chain(0, 3, q).wait_send()
            chain(1, 3, q).wait_send()

        @pl.when(jnp.logical_not(middle))
        def _():
            chain(z // 3, 3, q).wait_send()

    @pl.loop(0, G)
    def _(q):
        drain(line, across, q)

    @pl.loop(0, XG)
    def _(q):
        drain(x_line, x_across, q)
        for s in range(4):
            x_across(s, q).wait_recv()

    out.wait()


def gather_reduce(x, dy, pre, w_in, w_down):
    R, D = dy.shape
    rows, F = pre.shape
    T = F // G
    dma = pltpu.SemaphoreType.DMA
    any_spec = pl.BlockSpec(memory_space=pl.ANY)
    return pl.pallas_call(
        gather_reduce_kernel,
        name="gather_reduce",
        out_shape=(
            jax.ShapeDtypeStruct((rows, D), BF16),
            jax.ShapeDtypeStruct((rows, F), BF16),
            jax.ShapeDtypeStruct((rows, F), BF16),
            jax.ShapeDtypeStruct((R, D), BF16),
            jax.ShapeDtypeStruct((rows, XW * D // 7168), BF16),
            jax.ShapeDtypeStruct((R, XL * D // 7168), BF16),
            jax.ShapeDtypeStruct((R, D - (XW + XL) * D // 7168), BF16),
            jax.ShapeDtypeStruct((F, D), BF16),
        ),
        in_specs=[any_spec] * 5,
        out_specs=[any_spec] * 8,
        scratch_shapes=[
            pltpu.VMEM((4, R, D), F32),
            pltpu.VMEM((R, D), BF16),
            pltpu.VMEM((R, D), BF16),
            pltpu.VMEM((2, 2, R, D), BF16),
            pltpu.VMEM((2, R, D), BF16),
            dma((SLOTS, 2)),
            dma((4,)),
            dma((2, 2)),
            dma((2, 2)),
            dma((2, 3, G)),
            dma((4, G)),
            dma((4, G)),
            dma((4, G)),
            dma((2, 3, XG)),
            dma((4, XG)),
            dma((4, XG)),
            dma((4, XG)),
            dma((G,)),
            dma((G,)),
            dma((2, GC)),
            dma((2, 2, GC)),
            dma((2,)),
            dma((2,)),
            dma((2,)),
            pltpu.SemaphoreType.REGULAR,
        ],
        compiler_params=pltpu.CompilerParams(
            collective_id=0, has_side_effects=True, vmem_limit_bytes=VMEM
        ),
        cost_estimate=pl.CostEstimate(
            flops=4 * rows * D * F, bytes_accessed=16 * D * F, transcendentals=rows * F
        ),
    )(x, dy, pre, w_in, w_down)


def weight_grad_kernel(a, b, source, *rest, first, size, steps, small, aliased):
    if small:
        tiny, rest = rest[0], rest[1:]
    rest = rest[aliased:]
    o, target, rest = rest[0], rest[1], rest[2:]
    if small:
        tiny_out, *rest, tiny_buf, tiny_sem = rest
        tiny_in = pltpu.make_async_copy(tiny, tiny_buf, tiny_sem)
        tiny_out = pltpu.make_async_copy(tiny_buf, tiny_out, tiny_sem)
    buf, take, give = rest
    n = pl.program_id(0) * pl.num_programs(1) + pl.program_id(1)

    def part(i):
        return pl.ds(pl.multiple_of(first + i * size, size), size)

    def into(i):
        return pltpu.make_async_copy(source.at[part(i)], buf.at[i % 3], take.at[i % 3])

    def out(i):
        return pltpu.make_async_copy(buf.at[i % 3], target.at[part(i)], give.at[i % 3])

    @pl.when(n == 0)
    def _():
        into(n).start()
        if small:
            tiny_in.start()

    if small:

        @pl.when(n == 1)
        def _():
            tiny_in.wait()
            tiny_out.start()

    @pl.when(n >= 2)
    def _():
        out(n - 2).wait()

    @pl.when(n + 1 < steps)
    def _():
        into(n + 1).start()

    into(n).wait()
    out(n).start()
    o[...] = lax.dot_general(a[...], b[...], TN, preferred_element_type=F32).astype(BF16)

    @pl.when(n == steps - 1)
    def _():
        if steps > 1:
            out(n - 1).wait()
        out(n).wait()
        if small:
            tiny_out.wait()


def weight_grad(a, b, total, into, start, bm, bn, source, target, first, last, small=None):
    rows, A = a.shape
    B = b.shape[1]
    off, tall, wide = start // bm, A // bm, B // bn
    steps = tall * wide
    size = (last - first) // steps
    any_spec = pl.BlockSpec(memory_space=pl.ANY)
    args = [a, b, source]
    in_specs = [
        pl.BlockSpec((rows, bm), lambda j, i: (0, i)),
        pl.BlockSpec((rows, bn), lambda j, i: (0, j)),
        any_spec,
    ]
    out_shape = [jax.ShapeDtypeStruct((total, B), BF16), jax.ShapeDtypeStruct(source.shape, BF16)]
    out_specs = [pl.BlockSpec((bm, bn), lambda j, i: (i + off, j)), any_spec]
    if small is not None:
        args.append(small)
        in_specs.append(any_spec)
        out_shape.append(jax.ShapeDtypeStruct(small.shape, BF16))
        out_specs.append(any_spec)
    aliases = {}
    for n, array in enumerate((into, target)):
        if array is not None:
            aliases[len(args)] = n
            args.append(array)
            in_specs.append(any_spec)
    return pl.pallas_call(
        functools.partial(
            weight_grad_kernel,
            first=first, size=size, steps=steps, small=small is not None, aliased=len(aliases),
        ),
        name="weight_grad",
        grid=(wide, tall),
        out_shape=out_shape,
        in_specs=in_specs,
        out_specs=out_specs,
        scratch_shapes=[
            pltpu.VMEM((3, size, source.shape[1]), BF16),
            pltpu.SemaphoreType.DMA((3,)),
            pltpu.SemaphoreType.DMA((3,)),
        ]
        + ([] if small is None else [pltpu.VMEM(small.shape, BF16), pltpu.SemaphoreType.DMA]),
        input_output_aliases=aliases,
        compiler_params=pltpu.CompilerParams(
            dimension_semantics=("arbitrary", "arbitrary"), vmem_limit_bytes=VMEM
        ),
        cost_estimate=pl.CostEstimate(
            flops=2 * rows * A * B, bytes_accessed=2 * (rows * (A + B) + A * B), transcendentals=0
        ),
    )(*args)


WITH_X, NOUT = True, 8


def solution(mesh):
    def body(x, dy, pre, w_in, w_down):
        _, d_pre, _, dx, x_part, *late, down = gather_reduce(x, dy, pre, w_in, w_down)
        late = [lax.all_gather(piece, "tp", axis=0, tiled=True) for piece in late]
        D, F = w_in.shape
        dw_in, dw_down, dx = weight_grad(
            x_part, d_pre, D, None, 0, 512, 3584, down, None, 0, 2304, small=dx
        )
        dw_in, dw_down = weight_grad(
            late[0], d_pre, D, dw_in, XW, 512, 3584, down, dw_down, 2304, 3328
        )
        dw_in, dw_down = weight_grad(
            late[1], d_pre, D, dw_in, XW + XL, 512, 896, down, dw_down, 3328, F
        )
        return dx, dw_in, dw_down

    rows = P(("dp", "tp"), None)
    return jax.shard_map(
        body,
        mesh=mesh,
        in_specs=(rows, rows, P("dp", "tp"), P(None, "tp"), P("tp", None)),
        out_specs=(rows, P("dp", "tp"), P(("dp", "tp"), None)),
        check_vma=False,
    )
```

```python
import functools

import jax
import jax.numpy as jnp
from jax import lax
from jax.experimental import pallas as pl
from jax.experimental.pallas import tpu as pltpu
from jax.sharding import PartitionSpec as P

F32, BF16 = jnp.float32, jnp.bfloat16
NT = (((1,), (1,)), ((), ()))
TN = (((0,), (0,)), ((), ()))
G = 7
STRIP = 16
SLOTS = 4
VMEM = 67043328
XG = 9
GC = 14
BI, BJ = 4, 4
XG = 9
GC = 14
XL = 2560
NB = 5
XW = 4608
XL = 2048
C0 = 0.7978845608028654
C1 = 0.044715


def gather_reduce_kernel(
    x, dy, pre, w_in, w_down, dy_all, d_pre, hidden, dx, x_part, x_late0, x_late1, down,
    held, precv, psend, crecv, cs,
    ws, ios, hos, prs, ls, lr, ps, pr, xls, xlr, xps, xpr, pss, psr, css, csr, fas, fbs, fos, dxs, credit,
):
    R, D = dy.shape
    F = pre.shape[1]
    CH, T = D // G, F // G
    XC = x_part.shape[1] // XG
    t = lax.axis_index("tp")
    z, c = t // 2, t % 2
    partner = t + 1 - 2 * c

    def rows(s, core):
        return pl.ds(pl.multiple_of((2 * s + core) * R, R), R)

    def chunk(q):
        return pl.ds(pl.multiple_of(q * CH, CH), CH)

    def slab(q):
        return pl.ds(pl.multiple_of(q * (D // GC), D // GC), D // GC)

    def tile(j):
        return pl.ds(pl.multiple_of(j * T, T), T)

    def remote(src, dst, send, recv, to):
        return pltpu.make_async_remote_copy(
            src_ref=src, dst_ref=dst, send_sem=send, recv_sem=recv,
            device_id={"tp": to}, device_id_type=pl.DeviceIdType.MESH,
        )

    def line(way, hop, s, q, own=False):
        cols = pl.ds(0, D) if q is None else chunk(q)
        here = dy_all.at[rows(s, c), cols]
        src = dy.at[:, cols] if own else here
        return remote(src, here, ls.at[way, hop], lr.at[s, 0 if q is None else q], t + 2 - 4 * way)

    def across(s, q, own=False):
        cols = pl.ds(0, D) if q is None else chunk(q)
        here = dy_all.at[rows(s, c), cols]
        src = dy.at[:, cols] if own else here
        return remote(src, here, ps.at[s], pr.at[s], partner)

    def xcols(q):
        return pl.ds(0, XC * XG) if q is None else pl.ds(pl.multiple_of(q * XC, XC), XC)

    def x_line(way, hop, s, q, own=False):
        here = x_part.at[rows(s, c), xcols(q)]
        src = x.at[:, xcols(q)] if own else here
        return remote(src, here, xls.at[way, hop], xlr.at[s, 0 if q is None else q], t + 2 - 4 * way)

    def x_across(s, q, own=False):
        here = x_part.at[rows(s, c), xcols(q)]
        src = x.at[:, xcols(q)] if own else here
        return remote(src, here, xps.at[s], xpr.at[s], partner)

    def send_own(along, over, q):
        over(z, q, own=True).start()

        @pl.when(z < 3)
        def _():
            along(0, 0, z, q, own=True).start()

        @pl.when(z > 0)
        def _():
            along(1, 0, z, q, own=True).start()

    def pass_on(along, over, hop, q):
        @pl.when(z >= hop)
        def _():
            along(0, hop, z - hop, q).wait_recv()

            @pl.when(z < 3)
            def _():
                along(0, hop, z - hop, q).start()

            over(z - hop, q).start()

        @pl.when(z + hop <= 3)
        def _():
            along(1, hop, z + hop, q).wait_recv()

            @pl.when(z > 0)
            def _():
                along(1, hop, z + hop, q).start()

            over(z + hop, q).start()

    def drain(along, over):
        for hop in range(3):

            @pl.when(jnp.logical_and(z >= hop, z < 3))
            def _():
                along(0, hop, z, None).wait_send()

            @pl.when(jnp.logical_and(z + hop <= 3, z > 0))
            def _():
                along(1, hop, z, None).wait_send()

        for s in range(4):
            over(s, None).wait_send()

    def pair(k, g):
        return remote(
            psend.at[:, chunk(g)], precv.at[:, chunk(g)], pss.at[g], psr.at[g], partner
        )

    def chain(way, a, g):
        return remote(
            cs.at[way, :, slab(g)], crecv.at[way, (a - 1) % 2, :, slab(g)],
            css.at[way, g], csr.at[way, (a - 1) % 2, g], t + 2 - 4 * way,
        )

    def strips(step):
        @pl.loop(0, R // STRIP)
        def _(i):
            step(pl.ds(pl.multiple_of(i * STRIP, STRIP), STRIP))

    def pair_add(k, s, g):
        pair(k, g).wait_recv()
        source = jnp.logical_and(z % 3 == 0, k > 0)
        way = z // 3

        @pl.when(source)
        def _():
            @pl.when(jnp.logical_and(k == 3, g == 0))
            def _():
                pl.semaphore_wait(credit, 1)

            @pl.loop(0, GC // G)
            def _(j):
                piece = g * (GC // G) + j

                @pl.when(k >= 2)
                def _():
                    chain(way, k, piece).wait_send()

                def step(r):
                    total = held[s, r, slab(piece)] + precv[r, slab(piece)].astype(F32)
                    cs[way, r, slab(piece)] = total.astype(BF16)

                strips(step)
                chain(way, k, piece).start()

        @pl.when(jnp.logical_not(source))
        def _():
            def step(r):
                held[s, r, chunk(g)] += precv[r, chunk(g)].astype(F32)

            strips(step)

    def finished(g):
        return pltpu.make_async_copy(psend.at[:, slab(g)], dx.at[:, slab(g)], dxs.at[g])

    def arrive(way, a, g, forward, sent_before, last=False):
        d = a + way * (3 - 2 * a)
        chain(way, a, g).wait_recv()
        old = (a - 1) % 2
        if last:

            def step(r):
                total = held[d, r, slab(g)] + crecv[way, old, r, slab(g)].astype(F32)
                psend[r, slab(g)] = total.astype(BF16)

            strips(step)
            finished(g).start()
            return

        @pl.when(forward)
        def _():
            @pl.when(sent_before)
            def _():
                chain(way, a, g).wait_send()

            def step(r):
                total = held[d, r, slab(g)] + crecv[way, old, r, slab(g)].astype(F32)
                cs[way, r, slab(g)] = total.astype(BF16)

            strips(step)
            chain(way, a, g).start()

        @pl.when(jnp.logical_not(forward))
        def _():
            def step(r):
                held[d, r, slab(g)] += crecv[way, old, r, slab(g)].astype(F32)

            strips(step)

    middle = jnp.logical_and(z >= 1, z <= 2)
    ends = z % 3 == 0

    def hooks(k, v):
        @pl.when(jnp.logical_and(k < 3, v % 2 == 1))
        def _():
            pass_on(line, across, k + 1, v // 2)

        def x_pair(v, step):
            for j in range(2):

                @pl.when(jnp.logical_and(v >= 0, 2 * v + j < XG))
                def _():
                    step(2 * v + j)

        @pl.when(jnp.logical_or(jnp.logical_and(k == 1, ends), jnp.logical_and(k == 2, middle)))
        def _():
            x_pair(v, lambda q: send_own(x_line, x_across, q))

        @pl.when(jnp.logical_and(k == 2, middle))
        def _():
            x_pair(v - G, lambda q: pass_on(x_line, x_across, 1, q))

        @pl.when(jnp.logical_and(k == 3, middle))
        def _():
            x_pair(v, lambda q: pass_on(x_line, x_across, 2, q))

        @pl.when(jnp.logical_and(k >= 2, middle))
        def _():
            @pl.when(v == 0)
            def _():
                @pl.loop(0, 3)
                def _(g):
                    arrive(z - 1, k - 1, g, k == 3, False)

            @pl.when(v <= 10)
            def _():
                arrive(z - 1, k - 1, v + 3, k == 3, False)

    def tail_hooks(f):
        def sums(j, way, a, forward, sent_before, last=False):
            @pl.loop(0, 2)
            def _(i):
                arrive(way, a, 2 * j + i, forward, sent_before, last)

        @pl.when(middle)
        def _():
            @pl.when(f < 7)
            def _():
                sums(f, z - 1, 3, True, True)

            @pl.when(jnp.logical_and(jnp.logical_and(f >= 3, f <= 12), f % 3 < 2))
            def _():
                sums(2 * (f // 3 - 1) + f % 3, 2 - z, 3, True, False)

            @pl.when(jnp.logical_and(jnp.logical_and(f >= 5, f <= 11), f % 3 == 2))
            def _():
                @pl.loop(0, 5)
                def _(i):
                    g = 5 * (f // 3 - 1) + i

                    @pl.when(g < GC)
                    def _():
                        arrive(2 - z, 2, g, False, False, last=True)

        @pl.when(f == 1)
        def _():
            drain(line, across)

        @pl.when(f == 13)
        def _():
            drain(x_line, x_across)
            for s in range(4):
                x_across(s, None).wait_recv()

        @pl.when(ends)
        def _():
            def x_four(f, hop):
                for j in range(4):

                    @pl.when(4 * f + j < XG)
                    def _():
                        pass_on(x_line, x_across, hop, 4 * f + j)

            @pl.when(f < 3)
            def _():
                x_four(f, 1)

            @pl.when(jnp.logical_and(f >= 3, f < 6))
            def _():
                x_four(f - 3, 2)

            @pl.when(jnp.logical_and(f >= 9, f < 12))
            def _():
                x_four(f - 9, 3)

            @pl.when(jnp.logical_and(jnp.logical_and(f >= 8, f <= 15), f % 3 != 1))
            def _():
                sums(2 * ((f - 8) // 3) + (f - 8) % 3, (3 - z) // 3, 3, False, False, last=True)

    barrier = pltpu.get_barrier_semaphore()
    pl.semaphore_signal(barrier, inc=1, device_id={"tp": partner}, device_id_type=pl.DeviceIdType.MESH)

    @pl.when(z > 0)
    def _():
        pl.semaphore_signal(barrier, inc=1, device_id={"tp": t - 2}, device_id_type=pl.DeviceIdType.MESH)

    @pl.when(z < 3)
    def _():
        pl.semaphore_signal(barrier, inc=1, device_id={"tp": t + 2}, device_id_type=pl.DeviceIdType.MESH)


    @pl.when(middle)
    def _():
        pl.semaphore_wait(barrier, 3)

    @pl.when(jnp.logical_not(middle))
    def _():
        pl.semaphore_wait(barrier, 2)

    @pl.loop(0, G)
    def _(q):
        send_own(line, across, q)

    stage = pltpu.make_async_copy(x, psend, fos.at[0])
    stage.start()
    XP, XA = x_part.shape[1], x_late0.shape[1]
    staged = [
        pltpu.make_async_copy(psend.at[:, pl.ds(0, XP)], x_part.at[rows(z, c), :], fos.at[0]),
        pltpu.make_async_copy(psend.at[:, pl.ds(XP, XA)], x_late0, fos.at[1]),
        pltpu.make_async_copy(psend.at[:, pl.ds(XP + XA, D - XP - XA)], x_late1, fas.at[0]),
    ]

    mirror = z // 2
    u = z + mirror * (3 - 2 * z)

    def block(k):
        base = (k // 2) * k + (1 - k // 2) * ((k + u) % 2)
        return base + mirror * (3 - 2 * base)

    def passes(dyv, ring, dpre, hid, preb, acc):
        H = T // 2

        def load(src, lo, n, slot, part):
            return pltpu.make_async_copy(
                src, ring.at[slot, pl.ds(part * H, H), :], ws.at[slot, part]
            )

        def fetch(n):
            i, slot = n % 28, n % SLOTS

            @pl.when(n < 112)
            def _():
                for part in range(2):

                    @pl.when(i < 14)
                    def _():
                        src = w_down.at[
                            pl.ds(pl.multiple_of((i // 2) * T + part * H, H), H),
                            pl.ds(pl.multiple_of((i % 2) * F, F), F),
                        ]
                        load(src, 0, n, slot, part).start()

                    @pl.when(i >= 14)
                    def _():
                        src = w_in.at[pl.ds(pl.multiple_of((i - 14) * T + part * H, H), H), :]
                        load(src, 0, n, slot, part).start()

        def ready(n):
            slot = n % SLOTS
            for part in range(2):
                load(w_in.at[pl.ds(0, H), :], 0, n, slot, part).wait()
            return slot

        def pre_copies(s, m):
            return [
                pltpu.make_async_copy(
                    pre.at[rows(s, core), tile(m)], preb.at[m % 2, pl.ds(i * R, R), :], prs.at[m % 2, i]
                )
                for i, core in enumerate((c, 1 - c))
            ]

        def hid_copies(s, m):
            return [
                pltpu.make_async_copy(
                    hid.at[m % 2, pl.ds(i * R, R), :], hidden.at[rows(s, core), tile(m)], hos.at[m % 2, i]
                )
                for i, core in enumerate((c, 1 - c))
            ]

        def out_copies(s):
            return [
                pltpu.make_async_copy(dpre.at[pl.ds(i * R, R), :], d_pre.at[rows(s, core), :], ios.at[2 + i])
                for i, core in enumerate((c, 1 - c))
            ]

        for n in range(SLOTS):
            fetch(jnp.int32(n))

        @pl.loop(0, 4)
        def _(k):
            s = block(k)

            for cp in pre_copies(s, 0):
                cp.start()

            @pl.when(k == 0)
            def _():
                pltpu.make_async_copy(dy, dyv.at[pl.ds(0, R), :], ios.at[0]).start()

            @pl.when(k > 0)
            def _():
                pltpu.make_async_copy(dy_all.at[rows(s, c), :], dyv.at[pl.ds(0, R), :], ios.at[0]).start()

            across(s, None).wait_recv()

            other = pltpu.make_async_copy(dy_all.at[rows(s, 1 - c), :], dyv.at[pl.ds(R, R), :], ios.at[1])
            other.start()
            pltpu.make_async_copy(dy, dyv.at[pl.ds(0, R), :], ios.at[0]).wait()

            keep = pltpu.make_async_copy(dyv.at[pl.ds(0, R), :], dy_all.at[rows(s, c), :], ios.at[0])

            @pl.when(k == 0)
            def _():
                keep.start()
                stage.wait()
                for cp in staged:
                    cp.start()

            other.wait()

            @pl.loop(0, G)
            def _(m):
                n = 28 * k + 2 * m

                @pl.when(m < G - 1)
                def _():
                    for cp in pre_copies(s, m + 1):
                        cp.start()

                slot = ready(n)
                acc[...] = lax.dot_general(dyv[:, :F], ring[slot], NT, preferred_element_type=F32)
                fetch(n + SLOTS)
                slot = ready(n + 1)
                acc[...] += lax.dot_general(dyv[:, F:], ring[slot], NT, preferred_element_type=F32)
                fetch(n + 1 + SLOTS)
                for cp in pre_copies(s, m):
                    cp.wait()

                @pl.when(m >= 2)
                def _():
                    for cp in hid_copies(s, m - 2):
                        cp.wait()

                @pl.loop(0, 2 * R // STRIP)
                def _(i):
                    strip = pl.ds(pl.multiple_of(i * STRIP, STRIP), STRIP)
                    v = preb[m % 2, strip, :].astype(F32)
                    sq = v * v
                    th = jnp.tanh(v * (C0 + (C0 * C1) * sq))
                    cdf = 0.5 + 0.5 * th
                    slope = cdf + (v * (1.0 - th * th)) * (0.5 * C0 + (1.5 * C0 * C1) * sq)
                    dpre[strip, tile(m)] = (acc[strip, :] * slope).astype(BF16)
                    hid[m % 2, strip, :] = (v * cdf).astype(BF16)

                for cp in hid_copies(s, m):
                    cp.start()

                hooks(k, m)

                @pl.when(jnp.logical_and(m == 0, k > 0))
                def _():
                    pair_add(k - 1, block(k - 1), G - 1)

            @pl.when(k == 0)
            def _():
                keep.wait()
                for cp in staged:
                    cp.wait()

            for m in (G - 2, G - 1):
                for cp in hid_copies(s, m):
                    cp.wait()

            for cp in out_copies(s):
                cp.start()

            @pl.loop(0, G)
            def _(m):
                @pl.when(k > 0)
                def _():
                    pair(k - 1, m).wait_send()

                for half in range(2):
                    n = 28 * k + 14 + 2 * m + half
                    slot = ready(n)
                    term = lax.dot_general(dpre[...], ring[slot], NT, preferred_element_type=F32)
                    held[s, :, tile(2 * m + half)] = term[:R]
                    psend[:, tile(2 * m + half)] = term[R:].astype(BF16)
                    fetch(n + SLOTS)
                @pl.when(m > 0)
                def _():
                    pair_add(k, s, m - 1)

                pair(k, m).start()

                hooks(k, G + m)


            @pl.when(jnp.logical_and(k == 2, middle))
            def _():
                pl.semaphore_signal(
                    credit, inc=1, device_id={"tp": t - 2 + 4 * (z - 1)}, device_id_type=pl.DeviceIdType.MESH
                )

            @pl.when(k == 3)
            def _():
                pair_add(k, s, G - 1)

            for cp in out_copies(s):
                cp.wait()

    pl.run_scoped(
        passes,
        pltpu.VMEM((2 * R, D), BF16),
        pltpu.VMEM((SLOTS, T, F), BF16),
        pltpu.VMEM((2 * R, F), BF16),
        pltpu.VMEM((2, 2 * R, T), BF16),
        pltpu.VMEM((2, 2 * R, T), BF16),
        pltpu.VMEM((2 * R, T), F32),
    )

    @pl.loop(0, G)
    def _(g):
        pair(jnp.int32(3), g).wait_send()

    TI, TJ = F // BI, D // BJ

    def fill(fa, fb, fo):
        def strip(i, size):
            return pl.ds(pl.multiple_of(i * size, size), size)

        def a_copy(i):
            return pltpu.make_async_copy(hidden.at[:, strip(i, TI)], fa.at[i % 2], fas.at[i % 2])

        def b_copy(f):
            return pltpu.make_async_copy(dy_all.at[:, strip(f % BJ, TJ)], fb.at[f % 2], fbs.at[f % 2])

        def o_copy(f):
            return pltpu.make_async_copy(
                fo.at[f % 2], down.at[strip(f // BJ, TI), strip(f % BJ, TJ)], fos.at[f % 2]
            )

        a_copy(jnp.int32(0)).start()
        b_copy(jnp.int32(0)).start()

        @pl.loop(0, BI * BJ)
        def _(f):
            i = f // BJ

            @pl.when(f + 1 < BI * BJ)
            def _():
                b_copy(f + 1).start()

            @pl.when(f % BJ == 0)
            def _():
                @pl.when(i + 1 < BI)
                def _():
                    a_copy(i + 1).start()

                a_copy(i).wait()

            b_copy(f).wait()

            @pl.when(f >= 2)
            def _():
                o_copy(f - 2).wait()

            fo[f % 2] = lax.dot_general(
                fa[i % 2], fb[f % 2], TN, preferred_element_type=F32
            ).astype(BF16)
            o_copy(f).start()
            tail_hooks(f)

        for f in (BI * BJ - 2, BI * BJ - 1):
            o_copy(jnp.int32(f)).wait()

    pl.run_scoped(
        fill,
        pltpu.VMEM((2, 8 * R, TI), BF16),
        pltpu.VMEM((2, 8 * R, TJ), BF16),
        pltpu.VMEM((2, TI, TJ), BF16),
    )

    @pl.when(ends)
    def _():
        @pl.loop(GC - 2, GC)
        def _(g):
            arrive((3 - z) // 3, 3, g, False, False, last=True)

    @pl.loop(0, GC)
    def _(q):
        @pl.when(middle)
        def _():
            chain(0, 3, q).wait_send()
            chain(1, 3, q).wait_send()

        @pl.when(jnp.logical_not(middle))
        def _():
            chain(z // 3, 3, q).wait_send()

        finished(q).wait()


def gather_reduce(x, dy, pre, w_in, w_down):
    R, D = dy.shape
    rows, F = pre.shape
    T = F // G
    dma = pltpu.SemaphoreType.DMA
    any_spec = pl.BlockSpec(memory_space=pl.ANY)
    return pl.pallas_call(
        gather_reduce_kernel,
        name="gather_reduce",
        out_shape=(
            jax.ShapeDtypeStruct((rows, D), BF16),
            jax.ShapeDtypeStruct((rows, F), BF16),
            jax.ShapeDtypeStruct((rows, F), BF16),
            jax.ShapeDtypeStruct((R, D), BF16),
            jax.ShapeDtypeStruct((rows, XW * D // 7168), BF16),
            jax.ShapeDtypeStruct((R, XL * D // 7168), BF16),
            jax.ShapeDtypeStruct((R, D - (XW + XL) * D // 7168), BF16),
            jax.ShapeDtypeStruct((F, D), BF16),
        ),
        in_specs=[any_spec] * 5,
        out_specs=[any_spec] * 8,
        scratch_shapes=[
            pltpu.VMEM((4, R, D), F32),
            pltpu.VMEM((R, D), BF16),
            pltpu.VMEM((R, D), BF16),
            pltpu.VMEM((2, 2, R, D), BF16),
            pltpu.VMEM((2, R, D), BF16),
            dma((SLOTS, 2)),
            dma((4,)),
            dma((2, 2)),
            dma((2, 2)),
            dma((2, 3)),
            dma((4, G)),
            dma((4,)),
            dma((4,)),
            dma((2, 3)),
            dma((4, XG)),
            dma((4,)),
            dma((4,)),
            dma((G,)),
            dma((G,)),
            dma((2, GC)),
            dma((2, 2, GC)),
            dma((2,)),
            dma((2,)),
            dma((2,)),
            dma((GC,)),
            pltpu.SemaphoreType.REGULAR,
        ],
        compiler_params=pltpu.CompilerParams(
            collective_id=0, has_side_effects=True, vmem_limit_bytes=VMEM
        ),
        cost_estimate=pl.CostEstimate(
            flops=4 * rows * D * F, bytes_accessed=16 * D * F, transcendentals=rows * F
        ),
    )(x, dy, pre, w_in, w_down)


def weight_grad_kernel(a, b, source, *rest, first, size, steps, small, aliased):
    if small:
        tiny, rest = rest[0], rest[1:]
    rest = rest[aliased:]
    o, target, rest = rest[0], rest[1], rest[2:]
    if small:
        tiny_out, *rest, tiny_buf, tiny_sem = rest
        tiny_in = pltpu.make_async_copy(tiny, tiny_buf, tiny_sem)
        tiny_out = pltpu.make_async_copy(tiny_buf, tiny_out, tiny_sem)
    buf, take, give = rest
    n = pl.program_id(0) * pl.num_programs(1) + pl.program_id(1)

    def part(i):
        return pl.ds(pl.multiple_of(first + i * size, size), size)

    def into(i):
        return pltpu.make_async_copy(source.at[part(i)], buf.at[i % 3], take.at[i % 3])

    def out(i):
        return pltpu.make_async_copy(buf.at[i % 3], target.at[part(i)], give.at[i % 3])

    @pl.when(n == 0)
    def _():
        into(n).start()
        if small:
            tiny_in.start()

    if small:

        @pl.when(n == 1)
        def _():
            tiny_in.wait()
            tiny_out.start()

    @pl.when(n >= 2)
    def _():
        out(n - 2).wait()

    @pl.when(n + 1 < steps)
    def _():
        into(n + 1).start()

    into(n).wait()
    out(n).start()
    o[...] = lax.dot_general(a[...], b[...], TN, preferred_element_type=F32).astype(BF16)

    @pl.when(n == steps - 1)
    def _():
        out(n - 1).wait()
        out(n).wait()
        if small:
            tiny_out.wait()


def plain_grad_kernel(a, b, into, o):
    o[...] = lax.dot_general(a[...], b[...], TN, preferred_element_type=F32).astype(BF16)


def plain_grad(a, b, into, start, bm, bn):
    rows, A = a.shape
    B = b.shape[1]
    off = start // bm
    return pl.pallas_call(
        plain_grad_kernel,
        name="plain_grad",
        grid=(B // bn, A // bm),
        out_shape=jax.ShapeDtypeStruct(into.shape, BF16),
        in_specs=[
            pl.BlockSpec((rows, bm), lambda j, i: (0, i)),
            pl.BlockSpec((rows, bn), lambda j, i: (0, j)),
            pl.BlockSpec(memory_space=pl.ANY),
        ],
        out_specs=pl.BlockSpec((bm, bn), lambda j, i: (i + off, j)),
        input_output_aliases={2: 0},
        compiler_params=pltpu.CompilerParams(
            dimension_semantics=("arbitrary", "arbitrary"), vmem_limit_bytes=VMEM
        ),
        cost_estimate=pl.CostEstimate(
            flops=2 * rows * A * B, bytes_accessed=2 * (rows * (A + B) + A * B), transcendentals=0
        ),
    )(a, b, into)


def weight_grad(a, b, total, into, start, bm, bn, source, target, first, last, small=None):
    rows, A = a.shape
    B = b.shape[1]
    off, tall, wide = start // bm, A // bm, B // bn
    steps = tall * wide
    size = (last - first) // steps
    any_spec = pl.BlockSpec(memory_space=pl.ANY)
    args = [a, b, source]
    in_specs = [
        pl.BlockSpec((rows, bm), lambda j, i: (0, i)),
        pl.BlockSpec((rows, bn), lambda j, i: (0, j)),
        any_spec,
    ]
    out_shape = [jax.ShapeDtypeStruct((total, B), BF16), jax.ShapeDtypeStruct(source.shape, BF16)]
    out_specs = [pl.BlockSpec((bm, bn), lambda j, i: (i + off, j)), any_spec]
    if small is not None:
        args.append(small)
        in_specs.append(any_spec)
        out_shape.append(jax.ShapeDtypeStruct(small.shape, BF16))
        out_specs.append(any_spec)
    aliases = {}
    for n, array in enumerate((into, target)):
        if array is not None:
            aliases[len(args)] = n
            args.append(array)
            in_specs.append(any_spec)
    return pl.pallas_call(
        functools.partial(
            weight_grad_kernel,
            first=first, size=size, steps=steps, small=small is not None, aliased=len(aliases),
        ),
        name="weight_grad",
        grid=(wide, tall),
        out_shape=out_shape,
        in_specs=in_specs,
        out_specs=out_specs,
        scratch_shapes=[
            pltpu.VMEM((3, size, source.shape[1]), BF16),
            pltpu.SemaphoreType.DMA((3,)),
            pltpu.SemaphoreType.DMA((3,)),
        ]
        + ([] if small is None else [pltpu.VMEM(small.shape, BF16), pltpu.SemaphoreType.DMA]),
        input_output_aliases=aliases,
        compiler_params=pltpu.CompilerParams(
            dimension_semantics=("arbitrary", "arbitrary"), vmem_limit_bytes=VMEM
        ),
        cost_estimate=pl.CostEstimate(
            flops=2 * rows * A * B, bytes_accessed=2 * (rows * (A + B) + A * B), transcendentals=0
        ),
    )(*args)


WITH_X, NOUT = True, 8


def solution(mesh):
    def body(x, dy, pre, w_in, w_down):
        _, d_pre, _, dx, x_part, *late, down = gather_reduce(x, dy, pre, w_in, w_down)
        late = [lax.all_gather(piece, "tp", axis=0, tiled=True) for piece in late]
        D, F = w_in.shape
        dw_in, dw_down, dx = weight_grad(
            x_part, d_pre, D, None, 0, 512, 3584, down, None, 0, 2304, small=dx
        )
        dw_in, dw_down = weight_grad(
            late[0], d_pre, D, dw_in, XW, 512, 3584, down, dw_down, 2304, F
        )
        dw_in = plain_grad(late[1], d_pre, dw_in, XW + XL, 512, 1792)
        return dx, dw_in, dw_down

    rows = P(("dp", "tp"), None)
    return jax.shard_map(
        body,
        mesh=mesh,
        in_specs=(rows, rows, P("dp", "tp"), P(None, "tp"), P("tp", None)),
        out_specs=(rows, P("dp", "tp"), P(("dp", "tp"), None)),
        check_vma=False,
    )
```
